16 devices in a mesh: dp: 2 (over y, z), tp: 8 (over x, core).
Axes of the slice: x: 4, y: 2, z: 1, core: 2. Of those that a mesh axis runs over, the one named last changes fastest.
The devices are a block of a 4x4x8 slice.
Arguments:
- x: bfloat16 [4096, 4096], P(('dp', 'tp')), parts along dimension 0
- dy: bfloat16 [4096, 4096], P(('dp', 'tp')), parts along dimension 0
- gate: bfloat16 [4096, 16384], P('dp', 'tp'), parts along dimension 0
- up: bfloat16 [4096, 16384], P('dp', 'tp'), parts along dimension 0
- w_gate: bfloat16 [4096, 16384], P(None, 'tp')
- w_up: bfloat16 [4096, 16384], P(None, 'tp')
- w_down: bfloat16 [16384, 4096], P('tp')
Outputs:
- output 1: bfloat16 [4096, 4096], P(('dp', 'tp')), parts along dimension 0
- output 2: bfloat16 [8192, 16384], P('dp', 'tp'), parts along dimension 0
- output 3: bfloat16 [8192, 16384], P('dp', 'tp'), parts along dimension 0
- output 4: bfloat16 [32768, 4096], P(('dp', 'tp')), parts along dimension 0
There are 2 independent parts. The reference program is written for one: setup_inputs(seed, part) draws one part's arguments, and reference() takes and returns one part's arrays. A program takes and returns all parts, laid end to end along the dimension named above; an argument that names none is the same for every part.
All inputs are finite; a program needn't handle non-finite values.
Results may differ from the reference program's by a relative error of at most 0.012.
Values are sent between devices in bfloat16 or wider.
A program may use at most 768 MiB of HBM per device.

```python
import jax
import jax.numpy as jnp

ROWS = 2048
D = 4096
FF = 16384


def act(gate, up):
    return jax.nn.silu(gate) * up


def setup_inputs(seed: int = 0, part: int = 0) -> dict:
    kx, ky, ka, kb, kg, ku, kd = jax.random.split(jax.random.key(seed), 7)
    kx, ky, ka, kb = (jax.random.fold_in(k, part) for k in (kx, ky, ka, kb))
    drawn = {
        "x": jax.random.normal(kx, (ROWS, D), jnp.float32),
        "dy": jax.random.normal(ky, (ROWS, D), jnp.float32),
        "gate": jax.random.normal(ka, (ROWS, FF), jnp.float32),
        "up": jax.random.normal(kb, (ROWS, FF), jnp.float32),
        "w_gate": jax.random.normal(kg, (D, FF), jnp.float32) * D**-0.5,
        "w_up": jax.random.normal(ku, (D, FF), jnp.float32) * D**-0.5,
        "w_down": jax.random.normal(kd, (FF, D), jnp.float32) * FF**-0.5,
    }
    return {k: v.astype(jnp.bfloat16) for k, v in drawn.items()}


def reference(x, dy, gate, up, w_gate, w_up, w_down):
    hidden, back = jax.vjp(act, gate.astype(jnp.float32), up.astype(jnp.float32))
    d_hidden = jnp.dot(dy, w_down.T, preferred_element_type=jnp.float32)
    d_gate, d_up = (g.astype(jnp.bfloat16) for g in back(d_hidden))
    dx = jnp.dot(d_gate, w_gate.T, preferred_element_type=jnp.float32) + jnp.dot(d_up, w_up.T, preferred_element_type=jnp.float32)
    dw_gate = jnp.dot(x.T, d_gate, preferred_element_type=jnp.float32)
    dw_up = jnp.dot(x.T, d_up, preferred_element_type=jnp.float32)
    dw_down = jnp.dot(hidden.astype(jnp.bfloat16).T, dy, preferred_element_type=jnp.float32)
    return tuple(g.astype(jnp.bfloat16) for g in (dx, dw_gate, dw_up, dw_down))
```

```python
import functools

import jax
import jax.numpy as jnp
from jax import lax
from jax.experimental import pallas as pl
from jax.experimental.pallas import tpu as pltpu
from jax.sharding import PartitionSpec as P

BF16, F32 = jnp.bfloat16, jnp.float32
NT = (((1,), (1,)), ((), ()))
TN = (((0,), (0,)), ((), ()))
VMEM_LIMIT = 67043328
TILE = 1024


def dot(a, b, dims):
    return lax.dot_general(a, b, dims, preferred_element_type=F32)


def gather_kernel(
    chips,
    dy, x, gate, up, w_gate, w_up, w_down,
    dy_all, x_all, d_gate, d_up, hidden, dx_term,
    dy_tile, w_tile, act_tile, grads, hid, dx_tile, x_own,
    send_sem, recv_sem, w_sem, dy_sem, act_sem, grads_sem, hid_sem, dx_sem, own_sem,
):
    rows, width = dy.shape
    half = rows // 2
    ff = w_down.shape[0]
    down_tiles, up_tiles = ff // TILE, width // TILE
    me = lax.axis_index("tp")
    chip, core = me // 2, me % 2
    right, left, far = (chip + 1) % chips, (chip + chips - 1) % chips, (chip + 2) % chips
    to_right, to_left, partner = right * 2 + core, left * 2 + core, chip * 2 + 1 - core

    def span(device, h):
        return pl.ds(pl.multiple_of(device * rows + h * half, half), half)

    plan = [
        (me, 0, True, to_right), (me, 1, True, to_left), (me, 1, True, to_right), (me, 0, True, to_left),
        (me, 0, True, partner), (me, 1, True, partner),
        (to_left, 0, False, to_right), (to_right, 1, False, to_left),
        (to_left, 0, False, partner), (to_right, 1, False, partner),
        (to_left, 1, False, partner), (to_right, 0, False, partner),
        (far * 2 + core, 0, False, partner), (far * 2 + core, 1, False, partner),
    ]

    def remote(which, k):
        mine, whole = ((dy, dy_all), (x, x_all))[which]
        device, h, own, target = plan[k]
        return pltpu.make_async_remote_copy(
            src_ref=mine.at[pl.ds(h * half, half)] if own else whole.at[span(device, h)],
            dst_ref=whole.at[span(device, h)],
            send_sem=send_sem.at[which, k],
            recv_sem=recv_sem.at[which, k],
            device_id={"tp": target},
            device_id_type=pl.DeviceIdType.MESH,
        )

    def send(which, *ks):
        for k in ks:
            remote(which, k).start()

    def arrived(which, *ks):
        for k in ks:
            remote(which, k).wait_recv()

    def piece(s, p):
        near = (left if p < 2 else right) * 2 * rows + (p % 2) * rows
        first = 0 if p < 2 else half
        near = near + jnp.where(s == 1, first, half - first)
        whole = jnp.where(s == 0, chip, far) * 2 * rows + p * half
        start = jnp.where((s == 1) | (s == 2), near, whole)
        return pl.ds(pl.multiple_of(start, half), half)

    def part(p):
        return pl.ds(p * half, half)

    def load_dy(s, slot):
        for p in range(4):
            pltpu.make_async_copy(dy_all.at[piece(s, p)], dy_tile.at[slot, part(p)], dy_sem.at[slot]).start()

    def wait_dy(slot):
        pltpu.make_async_copy(dy_all.at[pl.ds(0, 4 * half)], dy_tile.at[slot], dy_sem.at[slot]).wait()

    def load_act(s):
        for i in range(down_tiles):
            cols = pl.ds(i * TILE, TILE)
            for p in range(4):
                for j, a in enumerate((gate, up)):
                    pltpu.make_async_copy(
                        a.at[piece(s, p), cols], act_tile.at[i, part(p), pl.ds(j * TILE, TILE)], act_sem.at[i]
                    ).start()

    def wait_act(i):
        pltpu.make_async_copy(gate.at[pl.ds(0, 4 * half), pl.ds(0, 2 * TILE)], act_tile.at[i], act_sem.at[i]).wait()

    def load_down(i, slot):
        at = pl.ds(pl.multiple_of(i * TILE, TILE), TILE)
        pltpu.make_async_copy(w_down.at[at], w_tile.at[slot], w_sem.at[slot]).start()

    def load_up(i, slot):
        at = pl.ds(pl.multiple_of(i * TILE, TILE), TILE)
        for j, w in enumerate((w_gate, w_up)):
            pltpu.make_async_copy(w.at[at], w_tile.at[slot, :, pl.ds(j * ff, ff)], w_sem.at[slot]).start()

    def wait_w(slot):
        pltpu.make_async_copy(w_down.at[pl.ds(0, TILE)], w_tile.at[slot], w_sem.at[slot]).wait()

    own_rows = pl.ds(pl.multiple_of(core * rows, rows), rows)
    all_rows = pl.ds(pl.multiple_of(me * rows, rows), rows)
    own_dy_in = pltpu.make_async_copy(dy, dy_tile.at[0, own_rows], own_sem.at[0])
    own_dy_out = pltpu.make_async_copy(dy_tile.at[0, own_rows], dy_all.at[all_rows], own_sem.at[1])
    own_x_in = pltpu.make_async_copy(x, x_own, own_sem.at[2])
    own_x_out = pltpu.make_async_copy(x_own, x_all.at[all_rows], own_sem.at[3])
    partner_rows = pl.ds(pl.multiple_of((1 - core) * rows, rows), rows)
    partner_all = pl.ds(pl.multiple_of(partner * rows, rows), rows)
    partner_dy_in = pltpu.make_async_copy(dy_all.at[partner_all], dy_tile.at[0, partner_rows], own_sem.at[4])

    load_down(0, 0)
    own_dy_in.start()
    load_act(0)
    barrier = pltpu.get_barrier_semaphore()
    for target in (to_right, to_left, partner):
        pl.semaphore_signal(barrier, inc=1, device_id={"tp": target}, device_id_type=pl.DeviceIdType.MESH)
    pl.semaphore_wait(barrier, 3)
    send(0, 4, 5, 0, 1, 2, 3)
    own_x_in.start()
    own_dy_in.wait()
    own_dy_out.start()
    arrived(0, 4, 5)
    partner_dy_in.start()
    partner_dy_in.wait()

    def step(s, _):
        slot_dy = s % 2

        @pl.when(s > 0)
        def _():
            wait_dy(slot_dy)

        def down(i, _):
            wait_w(i)

            @pl.when(i == 0)
            def _():
                load_down(1, 1)

            @pl.when(i == 1)
            def _():
                load_up(0, 0)

            @pl.when((s == 3) & (i == 0))
            def _():
                arrived(1, 0, 1)
                send(1, 6, 7, 8, 9)

            wait_act(i)

            @pl.when((s > 0) & (i == 0))
            def _():
                pltpu.make_async_copy(grads, dy_all.at[pl.ds(0, 4 * half)], grads_sem).wait()
                pltpu.make_async_copy(hid, hidden.at[pl.ds(0, 4 * half)], hid_sem).wait()

            d_hidden = dot(dy_tile[slot_dy], w_tile[i], NT)
            g, u = act_tile[i, :, :TILE].astype(F32), act_tile[i, :, TILE:].astype(F32)
            sig = jax.nn.sigmoid(g)
            act = g * sig
            at = pl.multiple_of(i * TILE, TILE)
            grads[:, pl.ds(at, TILE)] = (d_hidden * u * (sig + act * (1.0 - sig))).astype(BF16)
            grads[:, pl.ds(ff + at, TILE)] = (d_hidden * act).astype(BF16)
            hid[:, pl.ds(at, TILE)] = (act * u).astype(BF16)
            return 0

        lax.fori_loop(0, down_tiles, down, 0)
        for p in range(4):
            to = piece(s, p)
            pltpu.make_async_copy(grads.at[part(p), pl.ds(0, ff)], d_gate.at[to], grads_sem).start()
            pltpu.make_async_copy(grads.at[part(p), pl.ds(ff, ff)], d_up.at[to], grads_sem).start()
            pltpu.make_async_copy(hid.at[part(p)], hidden.at[to], hid_sem).start()

        @pl.when(s < 3)
        def _():
            load_act(s + 1)

        def back(i, _):
            slot = i % 2
            wait_w(slot)

            @pl.when(i < up_tiles - 1)
            def _():
                load_up(i + 1, 1 - slot)

            @pl.when((i == up_tiles - 1) & (s < 3))
            def _():
                load_down(0, 1 - slot)

            @pl.when((s == 0) & (i == 2))
            def _():
                own_x_in.wait()
                own_x_out.start()
                arrived(0, 0, 1)
                send(0, 6, 7, 8, 9)
                send(1, 0, 1, 2, 3, 4, 5)

            @pl.when((s == 0) & (i == 3))
            def _():
                own_dy_out.wait()
                arrived(0, 8, 9)

            @pl.when((s == 1) & (i == 1))
            def _():
                arrived(0, 2, 3)
                send(0, 10, 11)

            @pl.when((s == 1) & (i == 3))
            def _():
                arrived(0, 10, 11)

            @pl.when((s == 2) & (i == 0))
            def _():
                arrived(0, 6, 7)
                send(0, 12, 13)

            @pl.when((s == 2) & (i == 3))
            def _():
                arrived(0, 12, 13)

            @pl.when((s < 3) & (i == 3))
            def _():
                load_dy(s + 1, 1 - slot_dy)

            @pl.when((s == 3) & (i == 2))
            def _():
                arrived(1, 2, 3)
                send(1, 10, 11)

            @pl.when((s > 0) | (i > 1))
            def _():
                wait_dx(slot)

            dx_tile[slot] = dot(grads[...], w_tile[slot], NT).astype(BF16)
            cols = pl.ds(pl.multiple_of(i * TILE, TILE), TILE)
            for p in range(4):
                pltpu.make_async_copy(dx_tile.at[slot, part(p)], dx_term.at[piece(s, p), cols], dx_sem.at[slot]).start()
            return 0

        def wait_dx(slot):
            pltpu.make_async_copy(dx_tile.at[slot], dx_term.at[pl.ds(0, 4 * half), pl.ds(0, TILE)], dx_sem.at[slot]).wait()

        lax.fori_loop(0, up_tiles, back, 0)

        @pl.when(s == 3)
        def _():
            wait_dx(0)
            wait_dx(1)

        return 0

    lax.fori_loop(0, 4, step, 0)
    pltpu.make_async_copy(grads, dy_all.at[pl.ds(0, 4 * half)], grads_sem).wait()
    pltpu.make_async_copy(hid, hidden.at[pl.ds(0, 4 * half)], hid_sem).wait()
    own_x_out.wait()
    arrived(1, 6, 7)
    send(1, 12, 13)
    arrived(1, 4, 5, 8, 9, 10, 11, 12, 13)
    for which in range(2):
        for k in range(len(plan)):
            remote(which, k).wait_send()


def gather_and_back(n, dy, x, gate, up, w_gate, w_up, w_down):
    rows, width = dy.shape
    ff = w_down.shape[0]
    group = rows * n
    any_ = pl.BlockSpec(memory_space=pl.ANY)
    wide = jax.ShapeDtypeStruct((group, width), BF16)
    narrow = jax.ShapeDtypeStruct((group, ff), BF16)
    sem = pltpu.SemaphoreType.DMA
    return pl.pallas_call(
        functools.partial(gather_kernel, n // 2),
        out_shape=[wide, wide, narrow, narrow, narrow, wide],
        in_specs=[any_] * 7,
        out_specs=[any_] * 6,
        scratch_shapes=[
            pltpu.VMEM((2, 2 * rows, width), BF16),
            pltpu.VMEM((2, TILE, width), BF16),
            pltpu.VMEM((2, 2 * rows, 2 * TILE), BF16),
            pltpu.VMEM((2 * rows, 2 * ff), BF16),
            pltpu.VMEM((2 * rows, ff), BF16),
            pltpu.VMEM((2, 2 * rows, TILE), BF16),
            pltpu.VMEM((rows, width), BF16),
            sem((2, 14)), sem((2, 14)), sem((2,)), sem((2,)), sem((2,)), sem, sem, sem((2,)), sem((5,)),
        ],
        compiler_params=pltpu.CompilerParams(collective_id=0, has_side_effects=True, vmem_limit_bytes=VMEM_LIMIT),
        cost_estimate=pl.CostEstimate(flops=6 * group * width * ff, bytes_accessed=16 * group * width, transcendentals=0),
        name="gather_and_back",
    )(dy, x, gate, up, w_gate, w_up, w_down)


def weight_grads(x, d_gate, d_up, hidden, dy, bm=1024, bn=1024):
    tokens, width = x.shape
    ff = d_gate.shape[1]
    nf, nd = ff // bn, width // bn
    first = (ff // bm) * nd
    total = first + (width // bm) * 2 * nf

    def a(t):
        return jnp.minimum(t, first - 1)

    def b(t):
        return jnp.maximum(t - first, 0)

    def gate_col(t):
        return jnp.minimum(b(t) % (2 * nf), nf - 1)

    def up_col(t):
        return jnp.maximum(b(t) % (2 * nf) - nf, 0)

    def kernel(x_ref, dg_ref, du_ref, hid_ref, dy_ref, og_ref, ou_ref, od_ref):
        t = pl.program_id(0)
        r = b(t) % (2 * nf)

        @pl.when(t < first)
        def _():
            od_ref[...] = dot(hid_ref[...], dy_ref[...], TN).astype(BF16)

        @pl.when((t >= first) & (r < nf))
        def _():
            og_ref[...] = dot(x_ref[...], dg_ref[...], TN).astype(BF16)

        @pl.when((t >= first) & (r >= nf))
        def _():
            ou_ref[...] = dot(x_ref[...], du_ref[...], TN).astype(BF16)

    return pl.pallas_call(
        kernel,
        grid=(total,),
        in_specs=[
            pl.BlockSpec((tokens, bm), lambda t: (0, b(t) // (2 * nf))),
            pl.BlockSpec((tokens, bn), lambda t: (0, gate_col(t))),
            pl.BlockSpec((tokens, bn), lambda t: (0, up_col(t))),
            pl.BlockSpec((tokens, bm), lambda t: (0, a(t) // nd)),
            pl.BlockSpec((tokens, bn), lambda t: (0, a(t) % nd)),
        ],
        out_specs=[
            pl.BlockSpec((bm, bn), lambda t: (b(t) // (2 * nf), gate_col(t))),
            pl.BlockSpec((bm, bn), lambda t: (b(t) // (2 * nf), up_col(t))),
            pl.BlockSpec((bm, bn), lambda t: (a(t) // nd, a(t) % nd)),
        ],
        out_shape=[
            jax.ShapeDtypeStruct((width, ff), BF16),
            jax.ShapeDtypeStruct((width, ff), BF16),
            jax.ShapeDtypeStruct((ff, width), BF16),
        ],
        compiler_params=pltpu.CompilerParams(dimension_semantics=("arbitrary",), vmem_limit_bytes=VMEM_LIMIT),
        cost_estimate=pl.CostEstimate(flops=6 * tokens * width * ff, bytes_accessed=16 * tokens * width, transcendentals=0),
        name="weight_grads",
    )(x, d_gate, d_up, hidden, dy)


def solution(mesh):
    n = mesh.shape["tp"]

    def step(x, dy, gate, up, w_gate, w_up, w_down):
        dy_all, x_all, d_gate, d_up, hidden, dx_term = gather_and_back(n, dy, x, gate, up, w_gate, w_up, w_down)
        dx = lax.psum_scatter(dx_term, "tp", scatter_dimension=0, tiled=True)
        dw_gate, dw_up, dw_down = weight_grads(x_all, d_gate, d_up, hidden, dy_all)
        return dx, dw_gate, dw_up, dw_down

    token, feature = P(("dp", "tp"), None), P("dp", "tp")
    return jax.shard_map(
        step,
        mesh=mesh,
        in_specs=(token, token, feature, feature, P(None, "tp"), P(None, "tp"), P("tp", None)),
        out_specs=(token, feature, feature, token),
        check_vma=False,
    )
```

```python
import functools

import jax
import jax.numpy as jnp
from jax import lax
from jax.experimental import pallas as pl
from jax.experimental.pallas import tpu as pltpu
from jax.sharding import PartitionSpec as P

BF16, F32 = jnp.bfloat16, jnp.float32
NT = (((1,), (1,)), ((), ()))
TN = (((0,), (0,)), ((), ()))
VMEM_LIMIT = 67043328
TILE = 1024


def dot(a, b, dims):
    return lax.dot_general(a, b, dims, preferred_element_type=F32)


def gather_kernel(
    chips,
    dy, x, gate, up, w_gate, w_up, w_down,
    dy_all, x_all, d_gate, d_up, hidden, dx_term, corner,
    dy_tile, w_tile, act_tile, grads, hid, dx_tile, x_own, corner_left, corner_right,
    send_sem, recv_sem, w_sem, dy_sem, act_sem, grads_sem, hid_sem, dx_sem, own_sem, corner_sem,
):
    rows, width = dy.shape
    half = rows // 2
    ff = w_down.shape[0]
    down_tiles, up_tiles = ff // TILE, width // TILE
    me = lax.axis_index("tp")
    chip, core = me // 2, me % 2
    right, left, far = (chip + 1) % chips, (chip + chips - 1) % chips, (chip + 2) % chips
    to_right, to_left, partner = right * 2 + core, left * 2 + core, chip * 2 + 1 - core

    def span(device, h):
        return pl.ds(pl.multiple_of(device * rows + h * half, half), half)

    plan = [
        (me, 0, True, to_right), (me, 1, True, to_left), (me, 1, True, to_right), (me, 0, True, to_left),
        (me, 0, True, partner), (me, 1, True, partner),
        (to_left, 0, False, to_right), (to_right, 1, False, to_left),
        (to_left, 0, False, partner), (to_right, 1, False, partner),
        (to_left, 1, False, partner), (to_right, 0, False, partner),
        (far * 2 + core, 0, False, partner), (far * 2 + core, 1, False, partner),
    ]

    def remote(which, k):
        mine, whole = ((dy, dy_all), (x, x_all))[which]
        device, h, own, target = plan[k]
        return pltpu.make_async_remote_copy(
            src_ref=mine.at[pl.ds(h * half, half)] if own else whole.at[span(device, h)],
            dst_ref=whole.at[span(device, h)],
            send_sem=send_sem.at[which, k],
            recv_sem=recv_sem.at[which, k],
            device_id={"tp": target},
            device_id_type=pl.DeviceIdType.MESH,
        )

    def send(which, *ks):
        for k in ks:
            remote(which, k).start()

    def arrived(which, *ks):
        for k in ks:
            remote(which, k).wait_recv()

    def piece(s, p):
        near = (left if p < 2 else right) * 2 * rows + (p % 2) * rows
        first = 0 if p < 2 else half
        near = near + jnp.where(s == 1, first, half - first)
        whole = jnp.where(s == 0, chip, far) * 2 * rows + p * half
        start = jnp.where((s == 1) | (s == 2), near, whole)
        return pl.ds(pl.multiple_of(start, half), half)

    def part(p):
        return pl.ds(p * half, half)

    def load_dy(s, slot):
        for p in range(4):
            pltpu.make_async_copy(dy_all.at[piece(s, p)], dy_tile.at[slot, part(p)], dy_sem.at[slot]).start()

    def wait_dy(slot):
        pltpu.make_async_copy(dy_all.at[pl.ds(0, 4 * half)], dy_tile.at[slot], dy_sem.at[slot]).wait()

    def load_act(s):
        for i in range(down_tiles):
            cols = pl.ds(i * TILE, TILE)
            for p in range(4):
                for j, a in enumerate((gate, up)):
                    pltpu.make_async_copy(
                        a.at[piece(s, p), cols], act_tile.at[i, part(p), pl.ds(j * TILE, TILE)], act_sem.at[i]
                    ).start()

    def wait_act(i):
        pltpu.make_async_copy(gate.at[pl.ds(0, 4 * half), pl.ds(0, 2 * TILE)], act_tile.at[i], act_sem.at[i]).wait()

    def load_down(i, slot):
        at = pl.ds(pl.multiple_of(i * TILE, TILE), TILE)
        pltpu.make_async_copy(w_down.at[at], w_tile.at[slot], w_sem.at[slot]).start()

    def load_up(i, slot):
        at = pl.ds(pl.multiple_of(i * TILE, TILE), TILE)
        for j, w in enumerate((w_gate, w_up)):
            pltpu.make_async_copy(w.at[at], w_tile.at[slot, :, pl.ds(j * ff, ff)], w_sem.at[slot]).start()

    def wait_w(slot):
        pltpu.make_async_copy(w_down.at[pl.ds(0, TILE)], w_tile.at[slot], w_sem.at[slot]).wait()

    def corner_in(k):
        if k == 0:
            return pltpu.make_async_copy(hidden.at[:, pl.ds(0, TILE)], corner_left, corner_sem.at[0])
        return pltpu.make_async_copy(dy_all.at[:, pl.ds((k - 1) * TILE, TILE)], corner_right.at[k - 1], corner_sem.at[k])

    own_rows = pl.ds(pl.multiple_of(core * rows, rows), rows)
    all_rows = pl.ds(pl.multiple_of(me * rows, rows), rows)
    own_dy_in = pltpu.make_async_copy(dy, dy_tile.at[0, own_rows], own_sem.at[0])
    own_dy_out = pltpu.make_async_copy(dy_tile.at[0, own_rows], dy_all.at[all_rows], own_sem.at[1])
    own_x_in = pltpu.make_async_copy(x, x_own, own_sem.at[2])
    own_x_out = pltpu.make_async_copy(x_own, x_all.at[all_rows], own_sem.at[3])
    partner_rows = pl.ds(pl.multiple_of((1 - core) * rows, rows), rows)
    partner_all = pl.ds(pl.multiple_of(partner * rows, rows), rows)
    partner_dy_in = pltpu.make_async_copy(dy_all.at[partner_all], dy_tile.at[0, partner_rows], own_sem.at[4])

    barrier = pltpu.get_barrier_semaphore()
    for target in (to_right, to_left, partner):
        pl.semaphore_signal(barrier, inc=1, device_id={"tp": target}, device_id_type=pl.DeviceIdType.MESH)
    load_down(0, 0)
    own_dy_in.start()
    pl.semaphore_wait(barrier, 3)
    send(0, 0, 1, 4, 5, 2, 3)
    load_act(0)
    own_x_in.start()
    own_dy_in.wait()
    own_dy_out.start()
    arrived(0, 4, 5)
    partner_dy_in.start()
    partner_dy_in.wait()

    def step(s, _):
        slot_dy = s % 2

        @pl.when(s > 0)
        def _():
            wait_dy(slot_dy)

        def down(i, _):
            wait_w(i)

            @pl.when(i == 0)
            def _():
                load_down(1, 1)

            @pl.when(i == 1)
            def _():
                load_up(0, 0)

            @pl.when((s == 3) & (i == 0))
            def _():
                arrived(1, 0, 1)
                send(1, 6, 7, 8, 9)

            wait_act(i)

            @pl.when((s > 0) & (i == 0))
            def _():
                pltpu.make_async_copy(grads, dy_all.at[pl.ds(0, 4 * half)], grads_sem).wait()
                pltpu.make_async_copy(hid, hidden.at[pl.ds(0, 4 * half)], hid_sem).wait()

            d_hidden = dot(dy_tile[slot_dy], w_tile[i], NT)
            g, u = act_tile[i, :, :TILE].astype(F32), act_tile[i, :, TILE:].astype(F32)
            sig = jax.nn.sigmoid(g)
            act = g * sig
            at = pl.multiple_of(i * TILE, TILE)
            grads[:, pl.ds(at, TILE)] = (d_hidden * u * (sig + act * (1.0 - sig))).astype(BF16)
            grads[:, pl.ds(ff + at, TILE)] = (d_hidden * act).astype(BF16)
            hid[:, pl.ds(at, TILE)] = (act * u).astype(BF16)
            return 0

        lax.fori_loop(0, down_tiles, down, 0)
        for p in range(4):
            to = piece(s, p)
            pltpu.make_async_copy(grads.at[part(p), pl.ds(0, ff)], d_gate.at[to], grads_sem).start()
            pltpu.make_async_copy(grads.at[part(p), pl.ds(ff, ff)], d_up.at[to], grads_sem).start()
            pltpu.make_async_copy(hid.at[part(p)], hidden.at[to], hid_sem).start()

        @pl.when(s < 3)
        def _():
            load_act(s + 1)

        def back(i, _):
            slot = i % 2
            wait_w(slot)

            @pl.when(i < up_tiles - 1)
            def _():
                load_up(i + 1, 1 - slot)

            @pl.when((i == up_tiles - 1) & (s < 3))
            def _():
                load_down(0, 1 - slot)

            @pl.when((s == 0) & (i == 2))
            def _():
                own_x_in.wait()
                own_x_out.start()
                arrived(0, 0, 1)
                send(0, 6, 7, 8, 9)
                send(1, 0, 1, 2, 3, 4, 5)

            @pl.when((s == 0) & (i == 3))
            def _():
                own_dy_out.wait()
                arrived(0, 8, 9)

            @pl.when((s == 1) & (i == 1))
            def _():
                arrived(0, 2, 3)
                send(0, 10, 11)

            @pl.when((s == 1) & (i == 3))
            def _():
                arrived(0, 10, 11)

            @pl.when((s == 2) & (i == 0))
            def _():
                arrived(0, 6, 7)
                send(0, 12, 13)

            @pl.when((s == 2) & (i == 3))
            def _():
                arrived(0, 12, 13)

            @pl.when((s < 3) & (i == 3))
            def _():
                load_dy(s + 1, 1 - slot_dy)

            @pl.when((s == 3) & (i == 2))
            def _():
                arrived(1, 2, 3)
                send(1, 10, 11)
                pltpu.make_async_copy(hid, hidden.at[pl.ds(0, 4 * half)], hid_sem).wait()
                for k in range(3):
                    corner_in(k).start()

            @pl.when((s > 0) | (i > 1))
            def _():
                wait_dx(slot)

            dx_tile[slot] = dot(grads[...], w_tile[slot], NT).astype(BF16)
            cols = pl.ds(pl.multiple_of(i * TILE, TILE), TILE)
            for p in range(4):
                pltpu.make_async_copy(dx_tile.at[slot, part(p)], dx_term.at[piece(s, p), cols], dx_sem.at[slot]).start()
            return 0

        def wait_dx(slot):
            pltpu.make_async_copy(dx_tile.at[slot], dx_term.at[pl.ds(0, 4 * half), pl.ds(0, TILE)], dx_sem.at[slot]).wait()

        lax.fori_loop(0, up_tiles, back, 0)

        @pl.when(s == 3)
        def _():
            wait_dx(0)
            wait_dx(1)

        return 0

    lax.fori_loop(0, 4, step, 0)
    pltpu.make_async_copy(grads, dy_all.at[pl.ds(0, 4 * half)], grads_sem).wait()
    own_x_out.wait()
    corner_in(0).wait()

    def corner_part(k, _):
        @pl.when(k == 0)
        def _():
            corner_in(1).wait()

        @pl.when(k == 1)
        def _():
            corner_in(2).wait()
            arrived(1, 6, 7)
            send(1, 12, 13)

        cols = pl.ds(pl.multiple_of(k * TILE, TILE), TILE)
        w_tile[0, :, cols] = dot(corner_left[...], corner_right[k], TN).astype(BF16)
        return 0

    lax.fori_loop(0, 2, corner_part, 0)
    corner_out = pltpu.make_async_copy(w_tile.at[0, :, pl.ds(0, 2 * TILE)], corner, corner_sem.at[3])
    corner_out.start()
    corner_out.wait()
    arrived(1, 4, 5, 8, 9, 10, 11, 12, 13)
    for which in range(2):
        for k in range(len(plan)):
            remote(which, k).wait_send()


def gather_and_back(n, dy, x, gate, up, w_gate, w_up, w_down):
    rows, width = dy.shape
    ff = w_down.shape[0]
    group = rows * n
    any_ = pl.BlockSpec(memory_space=pl.ANY)
    wide = jax.ShapeDtypeStruct((group, width), BF16)
    narrow = jax.ShapeDtypeStruct((group, ff), BF16)
    sem = pltpu.SemaphoreType.DMA
    return pl.pallas_call(
        functools.partial(gather_kernel, n // 2),
        out_shape=[wide, wide, narrow, narrow, narrow, wide, jax.ShapeDtypeStruct((TILE, 2 * TILE), BF16)],
        in_specs=[any_] * 7,
        out_specs=[any_] * 7,
        scratch_shapes=[
            pltpu.VMEM((2, 2 * rows, width), BF16),
            pltpu.VMEM((2, TILE, width), BF16),
            pltpu.VMEM((2, 2 * rows, 2 * TILE), BF16),
            pltpu.VMEM((2 * rows, 2 * ff), BF16),
            pltpu.VMEM((2 * rows, ff), BF16),
            pltpu.VMEM((2, 2 * rows, TILE), BF16),
            pltpu.VMEM((rows, width), BF16),
            pltpu.VMEM((group, TILE), BF16),
            pltpu.VMEM((2, group, TILE), BF16),
            sem((2, 14)), sem((2, 14)), sem((2,)), sem((2,)), sem((2,)), sem, sem, sem((2,)), sem((5,)), sem((4,)),
        ],
        compiler_params=pltpu.CompilerParams(collective_id=0, has_side_effects=True, vmem_limit_bytes=VMEM_LIMIT),
        cost_estimate=pl.CostEstimate(flops=6 * group * width * ff, bytes_accessed=16 * group * width, transcendentals=0),
        name="gather_and_back",
    )(dy, x, gate, up, w_gate, w_up, w_down)


def choose(t, values):
    out = values[0]
    for k in range(1, len(values)):
        if values[k] != values[k - 1]:
            out = jnp.where(t >= k, values[k], out)
    return out


def grads_kernel(
    x, d_gate, d_up, hidden, dy, corner, dw_gate, dw_up, dw_down, lhs, rhs, out, through, lhs_sem, rhs_sem, out_sem, corner_sem
):
    bm, bn = lhs.shape[2], rhs.shape[2]
    lefts = [(hidden, 1, 0), (hidden, 0, 1), (x, 0, 2), (x, 1, 0), (x, 2, 1), (x, 3, 2)]
    rights = [(dy, 0, 0), (dy, 1, 1), (d_gate, 0, 2), (d_up, 0, 0)]
    steps = [
        (0, 0, dw_down, 1, 0), (0, 1, dw_down, 1, 1), (1, 1, dw_down, 0, 1),
        (2, 2, dw_gate, 0, 0), (2, 3, dw_up, 0, 0), (3, 3, dw_up, 1, 0), (3, 2, dw_gate, 1, 0),
        (4, 2, dw_gate, 2, 0), (4, 3, dw_up, 2, 0), (5, 3, dw_up, 3, 0), (5, 2, dw_gate, 3, 0),
    ]

    def left(k):
        a, c, slot = lefts[k]
        return pltpu.make_async_copy(a.at[:, pl.ds(c * bm, bm)], lhs.at[slot], lhs_sem.at[slot])

    def right(k):
        a, c, slot = rights[k]
        return pltpu.make_async_copy(a.at[:, pl.ds(c * bn, bn)], rhs.at[slot], rhs_sem.at[slot])

    def store(t, slot):
        _, _, a, r, c = steps[t]
        return pltpu.make_async_copy(out.at[slot], a.at[pl.ds(r * bm, bm), pl.ds(c * bn, bn)], out_sem.at[slot])

    corner_in = pltpu.make_async_copy(corner, through, corner_sem.at[0])
    corner_out = pltpu.make_async_copy(through, dw_down.at[pl.ds(0, bm), pl.ds(0, bn)], corner_sem.at[1])
    starts = {
        0: [left(1), right(1)], 1: [left(2), right(2), corner_in], 2: [right(3), left(3)], 3: [left(4), corner_out], 5: [left(5)],
    }
    waits = {
        0: [left(0), right(0)], 1: [right(1)], 2: [left(1)], 3: [left(2), right(2), corner_in], 4: [right(3)],
        5: [left(3)], 7: [left(4)], 9: [left(5)],
    }
    left(0).start()
    right(0).start()

    def step(t, _):
        for k in range(len(steps)):
            if k in waits or k in starts:

                @pl.when(t == k)
                def _(k=k):
                    for copy in waits.get(k, ()):
                        copy.wait()
                    for copy in starts.get(k, ()):
                        copy.start()

        slot = t % 2

        @pl.when(t >= 2)
        def _():
            store(0, slot).wait()

        a = lhs[choose(t, [lefts[k[0]][2] for k in steps])]
        b = rhs[choose(t, [rights[k[1]][2] for k in steps])]
        out[slot] = dot(a, b, TN).astype(BF16)
        for k in range(len(steps)):

            @pl.when(t == k)
            def _(k=k):
                store(k, k % 2).start()

        return 0

    lax.fori_loop(0, len(steps), step, 0)
    store(0, 0).wait()
    store(0, 1).wait()
    corner_out.wait()


def weight_grads(x, d_gate, d_up, hidden, dy, corner):
    tokens, width = x.shape
    ff = d_gate.shape[1]
    bm, bn = 1024, 2048
    any_ = pl.BlockSpec(memory_space=pl.ANY)
    sem = pltpu.SemaphoreType.DMA
    return pl.pallas_call(
        grads_kernel,
        in_specs=[any_] * 6,
        out_specs=[any_] * 3,
        out_shape=[
            jax.ShapeDtypeStruct((width, ff), BF16),
            jax.ShapeDtypeStruct((width, ff), BF16),
            jax.ShapeDtypeStruct((ff, width), BF16),
        ],
        scratch_shapes=[
            pltpu.VMEM((3, tokens, bm), BF16),
            pltpu.VMEM((3, tokens, bn), BF16),
            pltpu.VMEM((2, bm, bn), BF16),
            pltpu.VMEM((bm, bn), BF16),
            sem((3,)), sem((3,)), sem((2,)), sem((2,)),
        ],
        compiler_params=pltpu.CompilerParams(vmem_limit_bytes=VMEM_LIMIT),
        cost_estimate=pl.CostEstimate(flops=6 * tokens * width * ff, bytes_accessed=16 * tokens * width, transcendentals=0),
        name="weight_grads",
    )(x, d_gate, d_up, hidden, dy, corner)


def solution(mesh):
    n = mesh.shape["tp"]

    def step(x, dy, gate, up, w_gate, w_up, w_down):
        dy_all, x_all, d_gate, d_up, hidden, dx_term, corner = gather_and_back(n, dy, x, gate, up, w_gate, w_up, w_down)
        dx = lax.psum_scatter(dx_term, "tp", scatter_dimension=0, tiled=True)
        dw_gate, dw_up, dw_down = weight_grads(x_all, d_gate, d_up, hidden, dy_all, corner)
        return dx, dw_gate, dw_up, dw_down

    token, feature = P(("dp", "tp"), None), P("dp", "tp")
    return jax.shard_map(
        step,
        mesh=mesh,
        in_specs=(token, token, feature, feature, P(None, "tp"), P(None, "tp"), P("tp", None)),
        out_specs=(token, feature, feature, token),
        check_vma=False,
    )
```

```python
import functools

import jax
import jax.numpy as jnp
from jax import lax
from jax.experimental import pallas as pl
from jax.experimental.pallas import tpu as pltpu
from jax.sharding import PartitionSpec as P

BF16, F32 = jnp.bfloat16, jnp.float32
NT = (((1,), (1,)), ((), ()))
TN = (((0,), (0,)), ((), ()))
VMEM_LIMIT = 67043328
TILE = 1024
PART = 256


def dot(a, b, dims):
    return lax.dot_general(a, b, dims, preferred_element_type=F32)


def gather_kernel(
    chips,
    dy, x, gate, up, w_gate, w_up, w_down,
    dy_all, x_all, d_gate, d_up, hidden, dx_term, corner,
    dy_tile, w_tile, act_tile, grads, hid, dx_tile, x_own, corner_left, corner_right,
    send_sem, recv_sem, w_sem, dy_sem, act_sem, grads_sem, hid_sem, dx_sem, own_sem, corner_sem,
):
    rows, width = dy.shape
    half = rows // 2
    ff = w_down.shape[0]
    down_tiles, up_tiles = ff // TILE, width // TILE
    me = lax.axis_index("tp")
    chip, core = me // 2, me % 2
    right, left, far = (chip + 1) % chips, (chip + chips - 1) % chips, (chip + 2) % chips
    to_right, to_left, partner = right * 2 + core, left * 2 + core, chip * 2 + 1 - core

    def span(device, h):
        return pl.ds(pl.multiple_of(device * rows + h * half, half), half)

    plan = [
        (me, 0, True, to_right), (me, 1, True, to_left), (me, 1, True, to_right), (me, 0, True, to_left),
        (me, 0, True, partner), (me, 1, True, partner),
        (to_left, 0, False, to_right), (to_right, 1, False, to_left),
        (to_left, 0, False, partner), (to_right, 1, False, partner),
        (to_left, 1, False, partner), (to_right, 0, False, partner),
        (far * 2 + core, 0, False, partner), (far * 2 + core, 1, False, partner),
    ]

    def remote(which, k):
        mine, whole = ((dy, dy_all), (x, x_all))[which]
        device, h, own, target = plan[k]
        landing = whole.at[span(device, h)]
        if which == 0 and k in (4, 5):
            landing = dy_tile.at[0, pl.ds(pl.multiple_of(core * rows + h * half, half), half)]
        return pltpu.make_async_remote_copy(
            src_ref=mine.at[pl.ds(h * half, half)] if own else whole.at[span(device, h)],
            dst_ref=landing,
            send_sem=send_sem.at[which, k],
            recv_sem=recv_sem.at[which, k],
            device_id={"tp": target},
            device_id_type=pl.DeviceIdType.MESH,
        )

    def send(which, *ks):
        for k in ks:
            remote(which, k).start()

    def arrived(which, *ks):
        for k in ks:
            remote(which, k).wait_recv()

    def piece(s, p):
        near = (left if p < 2 else right) * 2 * rows + (p % 2) * rows
        first = 0 if p < 2 else half
        near = near + jnp.where(s == 1, first, half - first)
        whole = jnp.where(s == 0, chip, far) * 2 * rows + p * half
        start = jnp.where((s == 1) | (s == 2), near, whole)
        return pl.ds(pl.multiple_of(start, half), half)

    def part(p):
        return pl.ds(p * half, half)

    def load_dy(s, slot):
        for p in range(4):
            pltpu.make_async_copy(dy_all.at[piece(s, p)], dy_tile.at[slot, part(p)], dy_sem.at[slot]).start()

    def wait_dy(slot):
        pltpu.make_async_copy(dy_all.at[pl.ds(0, 4 * half)], dy_tile.at[slot], dy_sem.at[slot]).wait()

    def load_act(s):
        for i in range(down_tiles):
            cols = pl.ds(i * TILE, TILE)
            for p in range(4):
                for j, a in enumerate((gate, up)):
                    pltpu.make_async_copy(
                        a.at[piece(s, p), cols], act_tile.at[i, part(p), pl.ds(j * TILE, TILE)], act_sem.at[i]
                    ).start()

    def wait_act(i):
        pltpu.make_async_copy(gate.at[pl.ds(0, 4 * half), pl.ds(0, 2 * TILE)], act_tile.at[i], act_sem.at[i]).wait()

    def load_down(i, slot):
        at = pl.ds(pl.multiple_of(i * TILE, TILE), TILE)
        pltpu.make_async_copy(w_down.at[at], w_tile.at[slot], w_sem.at[slot]).start()

    def load_up(i, slot):
        at = pl.ds(pl.multiple_of(i * TILE, TILE), TILE)
        for j, w in enumerate((w_gate, w_up)):
            pltpu.make_async_copy(w.at[at], w_tile.at[slot, :, pl.ds(j * ff, ff)], w_sem.at[slot]).start()

    def wait_w(slot):
        pltpu.make_async_copy(w_down.at[pl.ds(0, TILE)], w_tile.at[slot], w_sem.at[slot]).wait()

    def corner_in(k):
        if k == 0:
            return pltpu.make_async_copy(hidden.at[:, pl.ds(0, TILE)], corner_left, corner_sem.at[0])
        return pltpu.make_async_copy(dy_all.at[:, pl.ds((k - 1) * TILE, TILE)], corner_right.at[k - 1], corner_sem.at[k])

    own_rows = pl.ds(pl.multiple_of(core * rows, rows), rows)
    all_rows = pl.ds(pl.multiple_of(me * rows, rows), rows)
    chip_rows = pl.ds(pl.multiple_of(chip * 2 * rows, rows), 2 * rows)
    own_dy_in = pltpu.make_async_copy(dy, dy_tile.at[0, own_rows], own_sem.at[0])
    chip_dy_out = pltpu.make_async_copy(dy_tile.at[0], dy_all.at[chip_rows], own_sem.at[1])
    own_x_in = pltpu.make_async_copy(x, x_own, own_sem.at[2])
    own_x_out = pltpu.make_async_copy(x_own, x_all.at[all_rows], own_sem.at[3])

    barrier = pltpu.get_barrier_semaphore()
    for target in (to_right, to_left, partner):
        pl.semaphore_signal(barrier, inc=1, device_id={"tp": target}, device_id_type=pl.DeviceIdType.MESH)
    load_down(0, 0)
    own_dy_in.start()
    pl.semaphore_wait(barrier, 3)
    send(0, 0, 1, 4, 5, 2, 3)
    load_act(0)
    own_x_in.start()
    own_dy_in.wait()
    arrived(0, 4, 5)
    chip_dy_out.start()

    def step(s, _):
        slot_dy = s % 2

        @pl.when(s > 0)
        def _():
            wait_dy(slot_dy)

        def down(i, _):
            wait_w(i)

            @pl.when(i == 0)
            def _():
                load_down(1, 1)

            @pl.when(i == 1)
            def _():
                load_up(0, 0)

            @pl.when((s == 3) & (i == 0))
            def _():
                arrived(1, 0, 1)
                send(1, 6, 7, 8, 9)

            wait_act(i)

            @pl.when((s > 0) & (i == 0))
            def _():
                pltpu.make_async_copy(grads, dy_all.at[pl.ds(0, 4 * half)], grads_sem).wait()
                pltpu.make_async_copy(hid, hidden.at[pl.ds(0, 4 * half)], hid_sem).wait()

            for first in range(0, TILE, PART):
                d_hidden = dot(dy_tile[slot_dy], w_tile[i, first : first + PART], NT)
                g = act_tile[i, :, first : first + PART].astype(F32)
                u = act_tile[i, :, TILE + first : TILE + first + PART].astype(F32)
                sig = jax.nn.sigmoid(g)
                act = g * sig
                at = pl.multiple_of(i * TILE + first, PART)
                grads[:, pl.ds(at, PART)] = (d_hidden * u * (sig + act * (1.0 - sig))).astype(BF16)
                grads[:, pl.ds(ff + at, PART)] = (d_hidden * act).astype(BF16)
                hid[:, pl.ds(at, PART)] = (act * u).astype(BF16)
            return 0

        lax.fori_loop(0, down_tiles, down, 0)
        for p in range(4):
            to = piece(s, p)
            pltpu.make_async_copy(grads.at[part(p), pl.ds(0, ff)], d_gate.at[to], grads_sem).start()
            pltpu.make_async_copy(grads.at[part(p), pl.ds(ff, ff)], d_up.at[to], grads_sem).start()
            pltpu.make_async_copy(hid.at[part(p)], hidden.at[to], hid_sem).start()

        @pl.when(s < 3)
        def _():
            load_act(s + 1)

        def back(i, _):
            slot = i % 2
            wait_w(slot)

            @pl.when(i < up_tiles - 1)
            def _():
                load_up(i + 1, 1 - slot)

            @pl.when((i == up_tiles - 1) & (s < 3))
            def _():
                load_down(0, 1 - slot)

            @pl.when((s == 0) & (i == 2))
            def _():
                own_x_in.wait()
                own_x_out.start()
                arrived(0, 0, 1)
                send(0, 6, 7, 8, 9)
                send(1, 0, 1, 2, 3, 4, 5)

            @pl.when((s == 0) & (i == 3))
            def _():
                chip_dy_out.wait()
                arrived(0, 8, 9)

            @pl.when((s == 1) & (i == 1))
            def _():
                arrived(0, 2, 3)
                send(0, 10, 11)

            @pl.when((s == 1) & (i == 3))
            def _():
                arrived(0, 10, 11)

            @pl.when((s == 2) & (i == 0))
            def _():
                arrived(0, 6, 7)
                send(0, 12, 13)

            @pl.when((s == 2) & (i == 3))
            def _():
                arrived(0, 12, 13)

            @pl.when((s < 3) & (i == 3))
            def _():
                load_dy(s + 1, 1 - slot_dy)

            @pl.when((s == 3) & (i == 2))
            def _():
                arrived(1, 2, 3)
                send(1, 10, 11)
                pltpu.make_async_copy(hid, hidden.at[pl.ds(0, 4 * half)], hid_sem).wait()
                for k in range(3):
                    corner_in(k).start()

            @pl.when((s > 0) | (i > 1))
            def _():
                wait_dx(slot)

            dx_tile[slot] = dot(grads[...], w_tile[slot], NT).astype(BF16)
            cols = pl.ds(pl.multiple_of(i * TILE, TILE), TILE)
            for p in range(4):
                pltpu.make_async_copy(dx_tile.at[slot, part(p)], dx_term.at[piece(s, p), cols], dx_sem.at[slot]).start()
            return 0

        def wait_dx(slot):
            pltpu.make_async_copy(dx_tile.at[slot], dx_term.at[pl.ds(0, 4 * half), pl.ds(0, TILE)], dx_sem.at[slot]).wait()

        lax.fori_loop(0, up_tiles, back, 0)

        @pl.when(s == 3)
        def _():
            wait_dx(0)
            wait_dx(1)

        return 0

    lax.fori_loop(0, 4, step, 0)
    pltpu.make_async_copy(grads, dy_all.at[pl.ds(0, 4 * half)], grads_sem).wait()
    own_x_out.wait()
    corner_in(0).wait()

    def corner_part(k, _):
        @pl.when(k == 0)
        def _():
            corner_in(1).wait()

        @pl.when(k == 1)
        def _():
            corner_in(2).wait()
            arrived(1, 6, 7)
            send(1, 12, 13)

        cols = pl.ds(pl.multiple_of(k * TILE, TILE), TILE)
        w_tile[0, :, cols] = dot(corner_left[...], corner_right[k], TN).astype(BF16)
        return 0

    lax.fori_loop(0, 2, corner_part, 0)
    corner_out = pltpu.make_async_copy(w_tile.at[0, :, pl.ds(0, 2 * TILE)], corner, corner_sem.at[3])
    corner_out.start()
    corner_out.wait()
    arrived(1, 4, 5, 8, 9, 10, 11, 12, 13)
    for which in range(2):
        for k in range(len(plan)):
            remote(which, k).wait_send()


def gather_and_back(n, dy, x, gate, up, w_gate, w_up, w_down):
    rows, width = dy.shape
    ff = w_down.shape[0]
    group = rows * n
    any_ = pl.BlockSpec(memory_space=pl.ANY)
    wide = jax.ShapeDtypeStruct((group, width), BF16)
    narrow = jax.ShapeDtypeStruct((group, ff), BF16)
    sem = pltpu.SemaphoreType.DMA
    return pl.pallas_call(
        functools.partial(gather_kernel, n // 2),
        out_shape=[wide, wide, narrow, narrow, narrow, wide, jax.ShapeDtypeStruct((TILE, 2 * TILE), BF16)],
        in_specs=[any_] * 7,
        out_specs=[any_] * 7,
        scratch_shapes=[
            pltpu.VMEM((2, 2 * rows, width), BF16),
            pltpu.VMEM((2, TILE, width), BF16),
            pltpu.VMEM((2, 2 * rows, 2 * TILE), BF16),
            pltpu.VMEM((2 * rows, 2 * ff), BF16),
            pltpu.VMEM((2 * rows, ff), BF16),
            pltpu.VMEM((2, 2 * rows, TILE), BF16),
            pltpu.VMEM((rows, width), BF16),
            pltpu.VMEM((group, TILE), BF16),
            pltpu.VMEM((2, group, TILE), BF16),
            sem((2, 14)), sem((2, 14)), sem((2,)), sem((2,)), sem((2,)), sem, sem, sem((2,)), sem((4,)), sem((4,)),
        ],
        compiler_params=pltpu.CompilerParams(collective_id=0, has_side_effects=True, vmem_limit_bytes=VMEM_LIMIT),
        cost_estimate=pl.CostEstimate(flops=6 * group * width * ff, bytes_accessed=16 * group * width, transcendentals=0),
        name="gather_and_back",
    )(dy, x, gate, up, w_gate, w_up, w_down)


def choose(t, values):
    out = values[0]
    for k in range(1, len(values)):
        if values[k] != values[k - 1]:
            out = jnp.where(t >= k, values[k], out)
    return out


def grads_kernel(
    x, d_gate, d_up, hidden, dy, corner, dw_gate, dw_up, dw_down, lhs, rhs, out, through, lhs_sem, rhs_sem, out_sem, corner_sem
):
    bm, bn = lhs.shape[2], rhs.shape[2]
    lefts = [(hidden, 1, 0), (hidden, 0, 1), (x, 0, 2), (x, 1, 0), (x, 2, 1), (x, 3, 2)]
    rights = [(dy, 0, 0), (dy, 1, 1), (d_gate, 0, 2), (d_up, 0, 0)]
    steps = [
        (0, 0, dw_down, 1, 0), (0, 1, dw_down, 1, 1), (1, 1, dw_down, 0, 1),
        (2, 2, dw_gate, 0, 0), (2, 3, dw_up, 0, 0), (3, 3, dw_up, 1, 0), (3, 2, dw_gate, 1, 0),
        (4, 2, dw_gate, 2, 0), (4, 3, dw_up, 2, 0), (5, 3, dw_up, 3, 0), (5, 2, dw_gate, 3, 0),
    ]

    def left(k):
        a, c, slot = lefts[k]
        return pltpu.make_async_copy(a.at[:, pl.ds(c * bm, bm)], lhs.at[slot], lhs_sem.at[slot])

    def right(k):
        a, c, slot = rights[k]
        return pltpu.make_async_copy(a.at[:, pl.ds(c * bn, bn)], rhs.at[slot], rhs_sem.at[slot])

    def store(t, slot):
        _, _, a, r, c = steps[t]
        return pltpu.make_async_copy(out.at[slot], a.at[pl.ds(r * bm, bm), pl.ds(c * bn, bn)], out_sem.at[slot])

    corner_in = pltpu.make_async_copy(corner, through, corner_sem.at[0])
    corner_out = pltpu.make_async_copy(through, dw_down.at[pl.ds(0, bm), pl.ds(0, bn)], corner_sem.at[1])
    starts = {
        0: [left(1), right(1)], 1: [left(2), right(2), corner_in], 2: [right(3), left(3)], 3: [left(4), corner_out], 5: [left(5)],
    }
    waits = {
        0: [left(0), right(0)], 1: [right(1)], 2: [left(1)], 3: [left(2), right(2), corner_in], 4: [right(3)],
        5: [left(3)], 7: [left(4)], 9: [left(5)],
    }
    left(0).start()
    right(0).start()

    def step(t, _):
        for k in range(len(steps)):
            if k in waits or k in starts:

                @pl.when(t == k)
                def _(k=k):
                    for copy in waits.get(k, ()):
                        copy.wait()
                    for copy in starts.get(k, ()):
                        copy.start()

        slot = t % 2

        @pl.when(t >= 2)
        def _():
            store(0, slot).wait()

        a = lhs[choose(t, [lefts[k[0]][2] for k in steps])]
        b = rhs[choose(t, [rights[k[1]][2] for k in steps])]
        out[slot] = dot(a, b, TN).astype(BF16)
        for k in range(len(steps)):

            @pl.when(t == k)
            def _(k=k):
                store(k, k % 2).start()

        return 0

    lax.fori_loop(0, len(steps), step, 0)
    store(0, 0).wait()
    store(0, 1).wait()
    corner_out.wait()


def weight_grads(x, d_gate, d_up, hidden, dy, corner):
    tokens, width = x.shape
    ff = d_gate.shape[1]
    bm, bn = 1024, 2048
    any_ = pl.BlockSpec(memory_space=pl.ANY)
    sem = pltpu.SemaphoreType.DMA
    return pl.pallas_call(
        grads_kernel,
        in_specs=[any_] * 6,
        out_specs=[any_] * 3,
        out_shape=[
            jax.ShapeDtypeStruct((width, ff), BF16),
            jax.ShapeDtypeStruct((width, ff), BF16),
            jax.ShapeDtypeStruct((ff, width), BF16),
        ],
        scratch_shapes=[
            pltpu.VMEM((3, tokens, bm), BF16),
            pltpu.VMEM((3, tokens, bn), BF16),
            pltpu.VMEM((2, bm, bn), BF16),
            pltpu.VMEM((bm, bn), BF16),
            sem((3,)), sem((3,)), sem((2,)), sem((2,)),
        ],
        compiler_params=pltpu.CompilerParams(vmem_limit_bytes=VMEM_LIMIT),
        cost_estimate=pl.CostEstimate(flops=6 * tokens * width * ff, bytes_accessed=16 * tokens * width, transcendentals=0),
        name="weight_grads",
    )(x, d_gate, d_up, hidden, dy, corner)


def solution(mesh):
    n = mesh.shape["tp"]

    def step(x, dy, gate, up, w_gate, w_up, w_down):
        dy_all, x_all, d_gate, d_up, hidden, dx_term, corner = gather_and_back(n, dy, x, gate, up, w_gate, w_up, w_down)
        dx = lax.psum_scatter(dx_term, "tp", scatter_dimension=0, tiled=True)
        dw_gate, dw_up, dw_down = weight_grads(x_all, d_gate, d_up, hidden, dy_all, corner)
        return dx, dw_gate, dw_up, dw_down

    token, feature = P(("dp", "tp"), None), P("dp", "tp")
    return jax.shard_map(
        step,
        mesh=mesh,
        in_specs=(token, token, feature, feature, P(None, "tp"), P(None, "tp"), P("tp", None)),
        out_specs=(token, feature, feature, token),
        check_vma=False,
    )
```
